128 devices in a mesh: dp: 32 (over z_hi, y, x), fsdp: 4 (over z_lo, core).
Axes of the slice: x: 4, y: 4, z: 4 (z_hi: 2, z_lo: 2; z = z_hi * 2 + z_lo), core: 2. Of those that a mesh axis runs over, the one named last changes fastest.
Arguments:
- tokens: bfloat16 [16384, 4096], P('dp'), may hold values from -6 to 6
- counts: int32 [32], P('dp'), may hold values from 256 to 512, as said below
- patch_index: int32 [16384], P('dp'), may hold values from 0 to 255
- clip_limit: float32 [], replicated, may hold values from 1024 to 8192
- norm_gain: float32 [4, 4096], replicated, may hold values from 0.25 to 1.75
- params: float32 [4, 4096, 4096], P(None, 'dp', 'fsdp'), may hold values from -0.09375 to 0.09375
- moments: float32 [4, 4096, 4096], P(None, 'dp', 'fsdp'), may hold values from -0.3 to 0.3
- seconds: float32 [4, 4096, 4096], P(None, 'dp', 'fsdp'), may hold values from 0.05 to 1
- gradients: float32 [4, 4096, 4096], P(None, 'dp', 'fsdp'), may hold values from -48 to 48
Outputs:
- params_new: float32 [4, 4096, 4096], P(None, 'dp', 'fsdp')
- moments_new: float32 [4, 4096, 4096], P(None, 'dp', 'fsdp')
- seconds_new: float32 [4, 4096, 4096], P(None, 'dp', 'fsdp')
- mixed: bfloat16 [16384, 4096], P('dp', 'fsdp')
The draws below stay inside these ranges and needn't reach their ends.
Inputs may be any that keep to these rules, and one draw needn't show every extreme that they name: `counts`: at most 512, reached on some index of dp in every draw.
All inputs are finite; a program needn't handle non-finite values.
Results may differ from the reference program's by a relative error of at most 0.0095.
Values may be sent and summed in bfloat16 or wider, within the bound.
No kernel may reach another device: no remote copies, remote signals or barrier semaphores. Data moves between devices by JAX's collectives and lax.ppermute only.
A program may use at most 192 MiB of HBM per device.

```python
import math
import jax
import jax.numpy as jnp
from jax import lax

D = 4096
TOK_DEV = 512
LAYERS = 4
GRID = 16
STEP = 40
TOKENS = 16384
N_DP = 32


def draw_counts(key, part):
    drawn = jax.random.randint(key, (N_DP,), TOK_DEV // 2, TOK_DEV + 1)
    chosen = jax.random.randint(jax.random.fold_in(key, 3), (), 0, N_DP)
    return jnp.where(jnp.arange(N_DP) == chosen, TOK_DEV, drawn).astype(jnp.int32)


def draw_gradients(key, part):
    rising = jnp.arange(D, dtype=jnp.float32)[None, :, None] / D
    scaling = 1.0 + 2.0 * rising
    noise = jnp.clip(jax.random.normal(key, (LAYERS, D, D), jnp.float32), -6.0, 6.0)
    return scaling * noise


def with_ends(values, key, low, high):
    longest = values.shape.index(max(values.shape))
    spots = []
    for shift in (0, 1):
        where = [jax.random.randint(jax.random.fold_in(key, axis), (), 0, length) for axis, length in enumerate(values.shape)]
        where[longest] = (where[longest] + shift) % values.shape[longest]
        spots.append(tuple(where))
    return values.at[spots[0]].set(low).at[spots[1]].set(high)


def block_scale(own_key, shape, cuts, smallest, high):
    factor_of = 1.0
    for dim, shards_of in cuts:
        draws = jax.random.uniform(jax.random.fold_in(jax.random.fold_in(own_key, 6), dim), (shards_of,), jnp.float32, smallest / len(cuts), high / len(cuts))
        factor_of = factor_of * jnp.repeat(jnp.exp(draws), shape[dim] // shards_of).reshape((-1,) + (1,) * (len(shape) - 1 - dim))
    return factor_of


def normal_values(key, dims, deviation, limit, split=(), held_as=jnp.bfloat16):
    entries = jax.random.normal(key, dims, jnp.float32) * deviation
    if len(split) > 0:
        entries = block_scale(key, dims, split, -0.22, 0.18) * entries
    return jnp.clip(entries, min=-limit, max=limit).astype(held_as)


def setup_inputs(seed: int = 0) -> dict:
    seeds = jax.random.split(jax.random.key(seed), 10)
    tokens = normal_values(seeds[0], (TOKENS, D), 1.0, 6.0, ((0, 32),))
    counts = draw_counts(jax.random.fold_in(seeds[9], 71), 0)
    patch_index = with_ends(jax.random.randint(seeds[2], (TOKENS,), 0, GRID * GRID), jax.random.fold_in(seeds[2], 1), 0, (GRID * GRID) - 1).astype(jnp.int32)
    clip_limit = jnp.clip(jnp.exp(jax.random.uniform(seeds[3], (), jnp.float32, math.log(1024.0), math.log(8192.0))), 1024.0, 8192.0)
    norm_gain = jnp.clip(1.0 + 0.15 * jax.random.normal(seeds[4], (LAYERS, D), jnp.float32), 0.25, 1.75)
    params = normal_values(seeds[5], (LAYERS, D, D), D ** -0.5, 0.09375, ((1, 32), (2, 4)), jnp.float32)
    moments = normal_values(seeds[6], (LAYERS, D, D), 0.05, 0.3, ((1, 32), (2, 4)), jnp.float32)
    seconds = jnp.clip(jnp.exp(math.log(1.0) - 2.9957323 * jax.random.uniform(seeds[7], (LAYERS, D, D), jnp.float32) ** block_scale(seeds[7], (LAYERS, D, D), ((1, 32), (2, 4)), -0.2, 0.2)), 0.05, 1.0)
    gradients = draw_gradients(jax.random.fold_in(seeds[9], 71), 0)
    return dict(tokens=tokens, counts=counts, patch_index=patch_index, clip_limit=clip_limit, norm_gain=norm_gain, params=params, moments=moments, seconds=seconds, gradients=gradients)


beta_one = 0.9
beta_two = 0.95
adam_eps = 1e-08
learning_rate = 0.0024
weight_decay = 0.05
norm_eps = 1e-06

def position_code(patch_index):
    quarter = D // 4
    freqs = 1.0 / 10000.0 ** (jnp.arange(quarter, dtype=jnp.float32) / quarter)
    across = (patch_index // GRID).astype(jnp.float32)[:, None] * freqs[None, :]
    downward = (patch_index % GRID).astype(jnp.float32)[:, None] * freqs[None, :]
    return jnp.concatenate([jnp.sin(across), jnp.cos(across), jnp.sin(downward), jnp.cos(downward)], axis=1)

def layer_norm(stream, gain_row):
    centre = lax.optimization_barrier(jnp.mean(stream, axis=1, keepdims=True))
    shifted = stream - centre
    spread = lax.optimization_barrier(jnp.mean(shifted * shifted, axis=1, keepdims=True))
    return (shifted * lax.rsqrt(spread + norm_eps) * gain_row[None, :]).astype(jnp.bfloat16)

def adam_update(params, moments, seconds, gradients, factor):
    clipped = gradients * factor
    moments_new = beta_one * moments + (1.0 - beta_one) * clipped
    seconds_new = beta_two * seconds + (1.0 - beta_two) * clipped * clipped
    direction = moments_new / (1.0 - beta_one ** STEP) / (jnp.sqrt(seconds_new / (1.0 - beta_two ** STEP)) + adam_eps)
    params_new = params - learning_rate * (direction + weight_decay * params)
    return (params_new, moments_new, seconds_new)

def reference(tokens, counts, patch_index, clip_limit, norm_gain, params, moments, seconds, gradients):
    squares = jnp.sum(gradients * gradients)
    factor = jnp.minimum(1.0, clip_limit / (jnp.sqrt(squares) + 1e-06))
    params_new, moments_new, seconds_new = adam_update(params, moments, seconds, gradients, factor)
    weights = params_new.astype(jnp.bfloat16)
    slot = jnp.arange(TOKENS, dtype=jnp.int32) % TOK_DEV
    valid = (slot < jnp.repeat(counts, TOK_DEV, total_repeat_length=TOKENS))[:, None]
    stream = jnp.where(valid, tokens.astype(jnp.float32) + position_code(patch_index), 0.0)
    for current in range(LAYERS):
        normed = layer_norm(stream, norm_gain[current])
        branch = jnp.dot(normed, weights[current], preferred_element_type=jnp.float32).astype(jnp.bfloat16)
        stream = stream + branch.astype(jnp.float32)
    mixed = jnp.where(valid, stream, 0.0).astype(jnp.bfloat16)
    return (params_new, moments_new, seconds_new, mixed)
```

```python
import functools

import jax
import jax.numpy as jnp
from jax import lax
from jax.experimental import pallas as pl
from jax.experimental.pallas import tpu as pltpu
from jax.sharding import Mesh
from jax.sharding import PartitionSpec as P

D = 4096
LAYERS = 4
GRID = 16
STEP = 40
BLK = 128
FSDP = ("zl", "core")
DP = ("zh", "y", "x")
EVERY = ("zh", "y", "x", "zl", "core")

beta_one = 0.9
beta_two = 0.95
adam_eps = 1e-08
learning_rate = 0.0024
weight_decay = 0.05
norm_eps = 1e-06


def shift(x, axis, step, size=4):
    return lax.ppermute(x, axis, [(i, (i + step) % size) for i in range(size)])


def swap(x, axis):
    return lax.ppermute(x, axis, [(0, 1), (1, 0)])


def total(x):
    spread = jnp.broadcast_to(x.reshape(1, 1), (128, 128))
    return jnp.sum(lax.all_to_all(spread, EVERY, 0, 0, tiled=True)[:, 0])


def adam_update(params, moments, seconds, gradients, factor):
    clipped = gradients * factor
    moments_new = beta_one * moments + (1.0 - beta_one) * clipped
    seconds_new = beta_two * seconds + (1.0 - beta_two) * clipped * clipped
    direction = (
        moments_new
        / (1.0 - beta_one**STEP)
        / (jnp.sqrt(seconds_new / (1.0 - beta_two**STEP)) + adam_eps)
    )
    params_new = params - learning_rate * (direction + weight_decay * params)
    return (params_new, moments_new, seconds_new)


def position_code(patch_index):
    quarter = D // 4
    freqs = 1.0 / 10000.0 ** (jnp.arange(quarter, dtype=jnp.float32) / quarter)
    angle = jnp.arange(GRID, dtype=jnp.int32).astype(jnp.float32)[:, None] * freqs[None, :]
    table = jnp.concatenate([jnp.sin(angle), jnp.cos(angle)], axis=1)
    lanes = jnp.arange(GRID, dtype=jnp.int32)[None, :]
    pick = lambda at: jnp.dot(
        (at[:, None] == lanes).astype(jnp.float32), table, precision=lax.Precision.HIGHEST
    )
    return jnp.concatenate([pick(patch_index // GRID), pick(patch_index % GRID)], axis=1)


def one_ring(x, axis):
    half = x.shape[0] // 2
    from_prev = shift(x, axis, 1)
    from_next = shift(x, axis, -1)
    far_head = shift(from_prev[:half], axis, 1)
    far_tail = shift(from_next[half:], axis, -1)
    return [x, from_prev, from_next, far_head, far_tail]


def gather_rows(own, partner):
    pieces = []
    for block, first, second in ((own, "x", "y"), (partner, "y", "x")):
        line = jnp.concatenate(one_ring(block, first), axis=0)
        pieces += one_ring(line, second)
    return pieces


def row_blocks():
    zh, y, x = lax.axis_index("zh"), lax.axis_index("y"), lax.axis_index("x")
    order = (0, 3, 1, 2)
    wrap = lambda v, s: lax.rem(v + s, 4)
    found = []
    for outer in order:
        for inner in order:
            found.append(zh * 16 + wrap(y, outer) * 4 + wrap(x, inner))
    for outer in order:
        for inner in order:
            found.append((1 - zh) * 16 + wrap(y, inner) * 4 + wrap(x, outer))
    return jnp.stack(found).astype(jnp.int32)


def norm_body(n, rows_ref, cols_ref, stream_ref, gain_ref, *refs):
    branches, (stream_out, normed_ref) = refs[:n], refs[n:]
    if n:
        for j, branch in enumerate(branches):
            at = pl.ds(pl.multiple_of(cols_ref[j] * 1024, 1024), 1024)
            stream_out[:, at] = stream_ref[:, at] + branch[...].astype(jnp.float32)
        stream_ref = stream_out
    stream = stream_ref[...]
    centre = jnp.sum(stream, axis=1, keepdims=True) * (1.0 / D)
    shifted = stream - centre
    spread = jnp.sum(shifted * shifted, axis=1, keepdims=True) * (1.0 / D)
    scale = lax.rsqrt(spread + norm_eps)
    for j in range(D // BLK):
        at = pl.ds(pl.multiple_of(rows_ref[j] * BLK, BLK), BLK)
        piece = (stream_ref[:, at] - centre) * scale * gain_ref[:, at]
        normed_ref[:, j * BLK : (j + 1) * BLK] = piece.astype(jnp.bfloat16)


def norm(stream, branches, gain_row, rows, cols):
    n = len(branches)
    tile = 64
    smem = pl.BlockSpec(memory_space=pltpu.SMEM)
    wide = pl.BlockSpec((tile, D), lambda i: (i, 0))
    out_shape = (
        jax.ShapeDtypeStruct(stream.shape, jnp.float32),
        jax.ShapeDtypeStruct(stream.shape, jnp.bfloat16),
    )
    out_specs = (wide, wide)
    body = functools.partial(norm_body, n)
    if n == 0:
        out_shape, out_specs = out_shape[1], wide
        body = lambda r, c, s, g, o: norm_body(0, r, c, s, g, None, o)
    return pl.pallas_call(
        body,
        grid=(stream.shape[0] // tile,),
        in_specs=[smem, smem, wide, pl.BlockSpec((1, D), lambda i: (0, 0))]
        + [pl.BlockSpec((tile, 1024), lambda i: (i, 0))] * n,
        out_specs=out_specs,
        out_shape=out_shape,
        name="norm",
        cost_estimate=pl.CostEstimate(flops=40 * 1000 * 1000, transcendentals=0, bytes_accessed=24 << 20),
    )(rows, cols, stream, gain_row, *branches)


def matmul_body(n, normed_ref, *refs):
    weights, out_ref = refs[:n], refs[n]
    acc, at = None, 0
    for w in weights:
        part = jnp.dot(
            normed_ref[:, at : at + w.shape[0]], w[...], preferred_element_type=jnp.float32
        )
        acc = part if acc is None else acc + part
        at += w.shape[0]
    out_ref[...] = acc.astype(jnp.bfloat16)


def matmul(normed, pieces):
    wide = 256
    return pl.pallas_call(
        functools.partial(matmul_body, len(pieces)),
        grid=(1024 // wide,),
        in_specs=[pl.BlockSpec(normed.shape, lambda i: (0, 0))]
        + [pl.BlockSpec((p.shape[0], wide), lambda i: (0, i)) for p in pieces],
        out_specs=pl.BlockSpec((normed.shape[0], wide), lambda i: (0, i)),
        out_shape=jax.ShapeDtypeStruct((normed.shape[0], 1024), jnp.bfloat16),
        name="project",
        cost_estimate=pl.CostEstimate(flops=2 * 512 * 4096 * 1024, transcendentals=0, bytes_accessed=14 << 20),
    )(normed, *pieces)


def per_device(
    tokens, counts, patch_index, clip_limit, norm_gain, params, moments, seconds, gradients
):
    squares = total(jnp.sum(gradients * gradients))
    factor = jnp.minimum(1.0, clip_limit / (jnp.sqrt(squares) + 1e-06))
    params_new, moments_new, seconds_new = adam_update(params, moments, seconds, gradients, factor)
    weights = params_new.astype(jnp.bfloat16)

    tok_rows = tokens.shape[0]
    valid = lax.broadcasted_iota(jnp.int32, (tok_rows, 1), 0) < counts[0]
    stream = jnp.where(valid, tokens.astype(jnp.float32) + position_code(patch_index), 0.0)
    rows = row_blocks()
    zl, core = lax.axis_index("zl"), lax.axis_index("core")
    mine = zl * 2 + core
    cols = jnp.stack([mine, zl * 2 + 1 - core, (1 - zl) * 2 + core, (1 - zl) * 2 + 1 - core]).astype(jnp.int32)

    branches = []
    for current in range(LAYERS):
        own = weights[current]
        pieces = gather_rows(own, swap(own, "zh"))
        gain_row = norm_gain[current][None, :]
        if current == 0:
            normed = norm(stream, (), gain_row, rows, cols)
        else:
            stream, normed = norm(stream, branches, gain_row, rows, cols)
        branch = matmul(normed, pieces)
        if current + 1 < LAYERS:
            across = swap(branch, "zl")
            branches = (branch, swap(branch, "core"), across, swap(across, "core"))
    last = lax.dynamic_slice_in_dim(stream, mine * 1024, 1024, 1) + branch.astype(jnp.float32)
    mixed = jnp.where(valid, last, 0.0).astype(jnp.bfloat16)
    return (params_new, moments_new, seconds_new, mixed)


def solution(mesh):
    split = Mesh(mesh.devices.reshape(2, 4, 4, 2, 2), EVERY)
    return jax.shard_map(
        per_device,
        mesh=split,
        in_specs=(
            P(DP, None),
            P(DP),
            P(DP),
            P(),
            P(),
            P(None, DP, FSDP),
            P(None, DP, FSDP),
            P(None, DP, FSDP),
            P(None, DP, FSDP),
        ),
        out_specs=(P(None, DP, FSDP), P(None, DP, FSDP), P(None, DP, FSDP), P(DP, FSDP)),
        check_vma=False,
    )
```

```python
import functools

import jax
import jax.numpy as jnp
from jax import lax
from jax.experimental import pallas as pl
from jax.experimental.pallas import tpu as pltpu
from jax.sharding import Mesh
from jax.sharding import PartitionSpec as P

D = 4096
LAYERS = 4
GRID = 16
STEP = 40
BLK = 128
FSDP = ("zl", "core")
DP = ("zh", "y", "x")
EVERY = ("zh", "y", "x", "zl", "core")

beta_one = 0.9
beta_two = 0.95
adam_eps = 1e-08
learning_rate = 0.0024
weight_decay = 0.05
norm_eps = 1e-06


def shift(x, axis, step, size=4):
    return lax.ppermute(x, axis, [(i, (i + step) % size) for i in range(size)])


def swap(x, axis):
    return lax.ppermute(x, axis, [(0, 1), (1, 0)])


def total(x):
    spread = jnp.broadcast_to(x.reshape(1, 1), (128, 128))
    return jnp.sum(lax.all_to_all(spread, EVERY, 0, 0, tiled=True)[:, 0])


def adam_update(params, moments, seconds, gradients, factor):
    clipped = gradients * factor
    moments_new = beta_one * moments + (1.0 - beta_one) * clipped
    seconds_new = beta_two * seconds + (1.0 - beta_two) * clipped * clipped
    direction = (
        moments_new
        / (1.0 - beta_one**STEP)
        / (jnp.sqrt(seconds_new / (1.0 - beta_two**STEP)) + adam_eps)
    )
    params_new = params - learning_rate * (direction + weight_decay * params)
    return (params_new, moments_new, seconds_new)


def tables(lanes):
    quarter = D // 4
    freqs = 1.0 / 10000.0 ** (lanes[0].astype(jnp.float32) / quarter)
    angle = lanes[1].astype(jnp.float32)[:, None] * freqs[None, :]
    return jnp.concatenate([jnp.sin(angle), jnp.cos(angle)], axis=1)


def join_body(*refs):
    for j, out in enumerate(refs[4:]):
        for k, part in enumerate(refs[:4]):
            out[k * BLK : (k + 1) * BLK, :] = part[j]


def join(parts):
    n = parts[0].shape[0]
    wide = 512
    return pl.pallas_call(
        join_body,
        grid=(1024 // wide,),
        in_specs=[pl.BlockSpec((n, BLK, wide), lambda i: (0, 0, i))] * 4,
        out_specs=[pl.BlockSpec((4 * BLK, wide), lambda i: (0, i))] * n,
        out_shape=[jax.ShapeDtypeStruct((4 * BLK, 1024), jnp.bfloat16)] * n,
        compiler_params=pltpu.CompilerParams(vmem_limit_bytes=20 << 20),
        name="join",
    )(*parts)


def first_phase(x, axis, step):
    ahead = shift(x, axis, step)
    behind = shift(x, axis, -step)
    far = shift(ahead, axis, step)
    prev, next_ = (ahead, behind) if step == 1 else (behind, ahead)
    return join((x, prev, next_, far))


def row_blocks(zh, y, x):
    order = jnp.array([0, 3, 1, 2], jnp.int32)
    ys, xs = (y + order) % 4, (x + order) % 4
    first = zh * 16 + ys[:, None] * 4 + xs[None, :]
    second = (1 - zh) * 16 + ys[None, :] * 4 + xs[:, None]
    return jnp.concatenate([first.reshape(-1), second.reshape(-1)])


def group_columns(zl, core):
    flips = jnp.arange(4, dtype=jnp.int32)
    return (zl * 2 + core) ^ flips


def normalize(at, rows_ref, stream_ref, gain_ref, normed_ref):
    stream = stream_ref[at, :]
    centre = jnp.sum(stream, axis=1, keepdims=True) * (1.0 / D)
    shifted = stream - centre
    spread = jnp.sum(shifted * shifted, axis=1, keepdims=True) * (1.0 / D)
    scale = lax.rsqrt(spread + norm_eps)
    for j in range(D // BLK):
        col = pl.ds(pl.multiple_of(rows_ref[j] * BLK, BLK), BLK)
        piece = (stream_ref[at, col] - centre) * scale * gain_ref[:, col]
        normed_ref[at, j * BLK : (j + 1) * BLK] = piece.astype(jnp.bfloat16)


TILE = 64
HALF = 256


def tile_rows():
    return pl.ds(pl.multiple_of(pl.program_id(0) * TILE, TILE), TILE)


def embed_body(h, rows_ref, counts_ref, tokens_ref, patch_ref, table_ref, gain_ref, stream_ref, normed_ref):
    at = tile_rows()
    patch = patch_ref[...]
    lanes = lax.broadcasted_iota(jnp.int32, (TILE, GRID), 1)
    slot = lax.broadcasted_iota(jnp.int32, (TILE, 1), 0) + (h * HALF + pl.program_id(0) * TILE)
    valid = slot < counts_ref[0]
    for side, where in enumerate((patch >> 4, patch & 15)):
        pick = (where == lanes).astype(jnp.float32)
        code = jnp.dot(
            pick, table_ref[...], precision=lax.Precision.HIGHEST, preferred_element_type=jnp.float32
        )
        cols = slice(side * 2048, side * 2048 + 2048)
        value = tokens_ref[:, cols].astype(jnp.float32) + code
        stream_ref[at, cols] = jnp.where(valid, value, 0.0)
    normalize(at, rows_ref, stream_ref, gain_ref, normed_ref)


def norm_body(rows_ref, cols_ref, stream_in, b0, b1, b2, b3, gain_ref, stream_ref, normed_ref, *mine):
    at = tile_rows()
    for j, branch in enumerate((b0, b1, b2, b3)):
        col = pl.ds(pl.multiple_of(cols_ref[j] * 1024, 1024), 1024)
        stream_ref[at, col] = stream_in[at, col] + branch[...].astype(jnp.float32)
    normalize(at, rows_ref, stream_ref, gain_ref, normed_ref)
    if mine:
        col = pl.ds(pl.multiple_of(cols_ref[0] * 1024, 1024), 1024)
        mine[0][...] = stream_ref[at, col]


SMEM = pl.BlockSpec(memory_space=pltpu.SMEM)
VMEM = pl.BlockSpec(memory_space=pltpu.VMEM)
ROW = pl.BlockSpec((1, D), lambda i: (0, 0))


def embed(h, tokens, patch_index, counts, table, gain_row, rows):
    steps = HALF // TILE
    return pl.pallas_call(
        functools.partial(embed_body, h),
        grid=(steps,),
        in_specs=[
            SMEM,
            SMEM,
            pl.BlockSpec((TILE, D), lambda i: (h * steps + i, 0)),
            pl.BlockSpec((TILE, 1), lambda i: (h * steps + i, 0)),
            pl.BlockSpec((GRID, 2048), lambda i: (0, 0)),
            ROW,
        ],
        out_specs=(VMEM, VMEM),
        out_shape=(pltpu.VMEM((HALF, D), jnp.float32), pltpu.VMEM((HALF, D), jnp.bfloat16)),
        compiler_params=pltpu.CompilerParams(vmem_limit_bytes=16 << 20),
        name="embed",
    )(rows, counts, tokens, patch_index, table, gain_row)


def norm(stream, branches, gain_row, rows, cols, last):
    out_specs = [VMEM, VMEM]
    out_shape = [pltpu.VMEM((HALF, D), jnp.float32), pltpu.VMEM((HALF, D), jnp.bfloat16)]
    tile = pl.BlockSpec((TILE, 1024), lambda i: (i, 0))
    if last:
        out_specs.append(tile)
        out_shape.append(jax.ShapeDtypeStruct((HALF, 1024), jnp.float32))
    return pl.pallas_call(
        norm_body,
        grid=(HALF // TILE,),
        in_specs=[SMEM, SMEM, VMEM, tile, tile, tile, tile, ROW],
        out_specs=out_specs,
        out_shape=out_shape,
        input_output_aliases={2: 0},
        compiler_params=pltpu.CompilerParams(vmem_limit_bytes=12 << 20),
        name="norm",
    )(rows, cols, stream, *branches, gain_row)


def matmul_body(n, last, normed_ref, *refs):
    weights, rest = refs[:n], refs[n:]
    out_ref, held = rest[-2:]
    at = 0
    for w in weights:
        held[at : at + w.shape[0], :] = w[...]
        at += w.shape[0]
    branch = jnp.dot(normed_ref[...], held[...], preferred_element_type=jnp.float32)
    branch = branch.astype(jnp.bfloat16)
    if last is None:
        out_ref[...] = branch
        return
    stream_ref, counts_ref = rest[:2]
    slot = lax.broadcasted_iota(jnp.int32, (HALF, 1), 0) + last * HALF
    value = stream_ref[...] + branch.astype(jnp.float32)
    out_ref[...] = jnp.where(slot < counts_ref[0], value, 0.0).astype(jnp.bfloat16)


def matmul(normed, pieces, final=None):
    wide = 256
    n = len(pieces)
    operands = [normed, *pieces]
    in_specs = [VMEM] + [pl.BlockSpec((p.shape[0], wide), lambda i: (0, i)) for p in pieces]
    rows, at, aliases, h = HALF, 0, {}, None
    if final is not None:
        h, stream, counts, so_far = final
        rows, at = 2 * HALF, h
        operands += [stream, counts]
        in_specs += [pl.BlockSpec((HALF, wide), lambda i: (0, i)), SMEM]
        if so_far is not None:
            aliases = {len(operands): 0}
            operands.append(so_far)
            in_specs.append(pl.BlockSpec(memory_space=pl.ANY))
    return pl.pallas_call(
        functools.partial(matmul_body, n, h),
        grid=(1024 // wide,),
        in_specs=in_specs,
        out_specs=pl.BlockSpec((HALF, wide), lambda i: (at, i)),
        out_shape=jax.ShapeDtypeStruct((rows, 1024), jnp.bfloat16),
        scratch_shapes=[pltpu.VMEM((D, wide), jnp.bfloat16)],
        input_output_aliases=aliases,
        compiler_params=pltpu.CompilerParams(vmem_limit_bytes=16 << 20),
        name="project",
        cost_estimate=pl.CostEstimate(flops=2 * 256 * 4096 * 1024, transcendentals=0, bytes_accessed=11 << 20),
    )(*operands)


after = lambda x, *others: lax.optimization_barrier((x, *others))[0]


def per_device(
    tokens, counts, patch_index, clip_limit, norm_gain, params, moments, seconds, gradients
):
    squares = total(jnp.sum(gradients * gradients))
    places = jnp.stack([lax.axis_index(name) for name in EVERY]).astype(jnp.int32)
    lanes = (jnp.arange(D // 4, dtype=jnp.int32), jnp.arange(GRID, dtype=jnp.int32))
    squares, places, lanes, tokens, counts, patch_index, norm_gain = lax.optimization_barrier(
        (squares, places, lanes, tokens, counts, patch_index, norm_gain)
    )
    factor = jnp.minimum(1.0, clip_limit / (jnp.sqrt(squares) + 1e-06))
    head = adam_update(params[0], moments[0], seconds[0], gradients[0], factor)[0]
    head = head.astype(jnp.bfloat16)[None]
    params_new, moments_new, seconds_new = adam_update(params, moments, seconds, gradients, factor)
    rest = params_new[1:].astype(jnp.bfloat16)
    table = tables(lanes)
    rows, cols = row_blocks(*places[:3]), group_columns(*places[3:])

    partner = swap(head, "zh")
    lines = {}
    (line_a,) = first_phase(head, "x", 1)
    (line_b,) = first_phase(partner, "y", -1)
    lines[0] = (line_a, line_b)
    partner = swap(rest, "zh")

    near, far = {}, {}
    axis_of = ("y", "x")

    def open_layer(l, *waits):
        for color in (0, 1):
            x = after(lines[l][color], *waits) if waits else lines[l][color]
            for step in (1, -1):
                near[l, color, step] = shift(x, axis_of[color], step)

    def forward(l):
        step = 1 if l % 2 == 0 else -1
        for color in (0, 1):
            far[l, color] = [shift(near[l, color, step], axis_of[color], step)]

    def forward_both(l):
        for color in (0, 1):
            halves = []
            for step, part in ((1, slice(0, 256)), (-1, slice(256, 512))):
                halves.append(shift(near[l, color, step][part], axis_of[color], step))
            far[l, color] = halves

    open_layer(0)
    forward(0)
    line_a = first_phase(rest, "x", -1)
    line_b = first_phase(partner, "y", -1)
    for l in (1, 2, 3):
        lines[l] = (line_a[l - 1], line_b[l - 1])
    open_layer(1)
    forward(1)
    open_layer(2, near[1, 0, -1], near[1, 1, -1])
    forward(2)
    open_layer(3, near[2, 0, 1], near[2, 1, 1])
    forward_both(3)

    streams, branches = [None, None], [None, None]
    mixed = None
    patch_index = patch_index[:, None]
    for l in range(LAYERS):
        pieces = []
        for color in (0, 1):
            pieces += [lines[l][color], near[l, color, 1], near[l, color, -1], *far[l, color]]
        gain_row = norm_gain[l][None, :]
        last = l + 1 == LAYERS
        for h in (0, 1):
            if l == 0:
                streams[h], normed = embed(h, tokens, patch_index, counts, table, gain_row, rows)
            else:
                streams[h], normed, *mine = norm(
                    streams[h], branches[h], gain_row, rows, cols, last
                )
            if last:
                mixed = matmul(normed, pieces, (h, mine[0], counts, mixed))
                continue
            branch = matmul(normed, pieces)
            across = swap(branch, "zl")
            beside = swap(branch, "core")
            both = swap(across, "core")
            branches[h] = (branch, beside, across, both)
    return (params_new, moments_new, seconds_new, mixed)


def solution(mesh):
    split = Mesh(mesh.devices.reshape(2, 4, 4, 2, 2), EVERY)
    return jax.shard_map(
        per_device,
        mesh=split,
        in_specs=(
            P(DP, None),
            P(DP),
            P(DP),
            P(),
            P(),
            P(None, DP, FSDP),
            P(None, DP, FSDP),
            P(None, DP, FSDP),
            P(None, DP, FSDP),
        ),
        out_specs=(P(None, DP, FSDP), P(None, DP, FSDP), P(None, DP, FSDP), P(DP, FSDP)),
        check_vma=False,
    )
```

```python
import functools

import jax
import jax.numpy as jnp
from jax import lax
from jax.experimental import pallas as pl
from jax.experimental.pallas import tpu as pltpu
from jax.sharding import Mesh
from jax.sharding import PartitionSpec as P

D = 4096
LAYERS = 4
GRID = 16
STEP = 40
BLK = 128
FSDP = ("zl", "core")
DP = ("zh", "y", "x")
EVERY = ("zh", "y", "x", "zl", "core")

beta_one = 0.9
beta_two = 0.95
adam_eps = 1e-08
learning_rate = 0.0024
weight_decay = 0.05
norm_eps = 1e-06


def shift(x, axis, step, size=4):
    return lax.ppermute(x, axis, [(i, (i + step) % size) for i in range(size)])


def swap(x, axis):
    return lax.ppermute(x, axis, [(0, 1), (1, 0)])


def total(x):
    spread = jnp.broadcast_to(x.reshape(1, 1), (128, 128))
    return jnp.sum(lax.all_to_all(spread, EVERY, 0, 0, tiled=True)[:, 0])


def adam_update(params, moments, seconds, gradients, factor):
    clipped = gradients * factor
    moments_new = beta_one * moments + (1.0 - beta_one) * clipped
    seconds_new = beta_two * seconds + (1.0 - beta_two) * clipped * clipped
    direction = (
        moments_new
        / (1.0 - beta_one**STEP)
        / (jnp.sqrt(seconds_new / (1.0 - beta_two**STEP)) + adam_eps)
    )
    params_new = params - learning_rate * (direction + weight_decay * params)
    return (params_new, moments_new, seconds_new)


STRIP = 8


def hbm(x):
    return pltpu.with_memory_space_constraint(x, pltpu.MemorySpace.HBM)


def adam_body(factor_ref, *refs):
    weights_ref = refs[7]

    def strip(j, carry):
        at = pl.ds(pl.multiple_of(j * STRIP, STRIP), STRIP)
        new = adam_update(*[r[0, at, :] for r in refs[:4]], factor_ref[0])
        for ref, value in zip(refs[4:7], new):
            ref[0, at, :] = value
        return carry

    lax.fori_loop(0, refs[0].shape[1] // STRIP, strip, 0)
    weights_ref[...] = refs[4][...].astype(jnp.bfloat16)


def adam(params, moments, seconds, gradients, factor):
    rows = 64
    block = pl.BlockSpec((1, rows, 1024), lambda j, l: (l, j, 0))
    whole = jax.ShapeDtypeStruct(params.shape, jnp.float32)
    rest = jax.ShapeDtypeStruct((LAYERS - 1, BLK, 1024), jnp.bfloat16)
    return pl.pallas_call(
        adam_body,
        grid=(BLK // rows, LAYERS),
        in_specs=[pl.BlockSpec(memory_space=pltpu.SMEM)] + [block] * 4,
        out_specs=[block] * 3 + [pl.BlockSpec((1, rows, 1024), lambda j, l: (jnp.maximum(l - 1, 0), j, 0))],
        out_shape=[whole] * 3 + [rest],
        compiler_params=pltpu.CompilerParams(vmem_limit_bytes=12 << 20),
        name="adam",
    )(factor.reshape(1), *[hbm(x) for x in (params, moments, seconds, gradients)])


def tables(lanes):
    quarter = D // 4
    freqs = 1.0 / 10000.0 ** (lanes[0].astype(jnp.float32) / quarter)
    angle = lanes[1].astype(jnp.float32)[:, None] * freqs[None, :]
    table = jnp.concatenate([jnp.sin(angle), jnp.cos(angle)], axis=1)
    high = lax.reduce_precision(table, 8, 7)
    middle = lax.reduce_precision(table - high, 8, 7)
    low = table - high - middle
    return jnp.concatenate([high, middle, low], axis=0).astype(jnp.bfloat16)


def join_body(*refs):
    for j, out in enumerate(refs[4:]):
        for k, part in enumerate(refs[:4]):
            out[k * BLK : (k + 1) * BLK, :] = part[j]


def join(parts):
    n = parts[0].shape[0]
    wide = 512
    return pl.pallas_call(
        join_body,
        grid=(1024 // wide,),
        in_specs=[pl.BlockSpec((n, BLK, wide), lambda i: (0, 0, i))] * 4,
        out_specs=[pl.BlockSpec((4 * BLK, wide), lambda i: (0, i))] * n,
        out_shape=[jax.ShapeDtypeStruct((4 * BLK, 1024), jnp.bfloat16)] * n,
        compiler_params=pltpu.CompilerParams(vmem_limit_bytes=12 << 20),
        name="join",
    )(*parts)


def first_phase(x, axis, step):
    ahead = shift(x, axis, step)
    behind = shift(x, axis, -step)
    far = shift(ahead, axis, step)
    prev, next_ = (ahead, behind) if step == 1 else (behind, ahead)
    return join((x, prev, next_, far))


def row_blocks(zh, y, x):
    order = jnp.array([0, 3, 1, 2], jnp.int32)
    ys, xs = (y + order) % 4, (x + order) % 4
    first = zh * 16 + ys[:, None] * 4 + xs[None, :]
    second = (1 - zh) * 16 + ys[None, :] * 4 + xs[:, None]
    return jnp.concatenate([first.reshape(-1), second.reshape(-1)])


def group_columns(zl, core):
    flips = jnp.arange(4, dtype=jnp.int32)
    return (zl * 2 + core) ^ flips


def normalize(at, rows_ref, stream_ref, gain_ref, normed_ref):
    stream = stream_ref[at, :]
    centre = jnp.sum(stream, axis=1, keepdims=True) * (1.0 / D)
    shifted = stream - centre
    spread = jnp.sum(shifted * shifted, axis=1, keepdims=True) * (1.0 / D)
    scale = lax.rsqrt(spread + norm_eps)
    for j in range(D // BLK):
        col = pl.ds(pl.multiple_of(rows_ref[j] * BLK, BLK), BLK)
        piece = (stream_ref[at, col] - centre) * scale * gain_ref[:, col]
        normed_ref[at, j * BLK : (j + 1) * BLK] = piece.astype(jnp.bfloat16)


TILE = 64
HALF = 256


def tile_rows():
    return pl.ds(pl.multiple_of(pl.program_id(0) * TILE, TILE), TILE)


def embed_body(half_ref, rows_ref, counts_ref, tokens_ref, patch_ref, table_ref, gain_ref, stream_ref, normed_ref):
    at = tile_rows()
    patch = patch_ref[...]
    lanes = lax.broadcasted_iota(jnp.int32, (TILE, 3 * GRID), 1) & (GRID - 1)
    first = half_ref[0] * HALF + pl.program_id(0) * TILE
    valid = lax.broadcasted_iota(jnp.int32, (TILE, 1), 0) + first < counts_ref[0]
    for side, where in enumerate((patch >> 4, patch & (GRID - 1))):
        pick = jnp.where(where == lanes, 1.0, 0.0).astype(jnp.bfloat16)
        code = jnp.dot(pick, table_ref[...], preferred_element_type=jnp.float32)
        cols = slice(side * 2048, side * 2048 + 2048)
        value = tokens_ref[:, cols].astype(jnp.float32) + code
        stream_ref[at, cols] = jnp.where(valid, value, 0.0)
    normalize(at, rows_ref, stream_ref, gain_ref, normed_ref)


def norm_body(rows_ref, cols_ref, stream_in, b0, b1, b2, b3, gain_ref, stream_ref, normed_ref, *mine):
    at = tile_rows()
    for j, branch in enumerate((b0, b1, b2, b3)):
        col = pl.ds(pl.multiple_of(cols_ref[j] * 1024, 1024), 1024)
        stream_ref[at, col] = stream_in[at, col] + branch[...].astype(jnp.float32)
    normalize(at, rows_ref, stream_ref, gain_ref, normed_ref)
    if mine:
        col = pl.ds(pl.multiple_of(cols_ref[0] * 1024, 1024), 1024)
        mine[0][...] = stream_ref[at, col]


SMEM = pl.BlockSpec(memory_space=pltpu.SMEM)
VMEM = pl.BlockSpec(memory_space=pltpu.VMEM)
ROW = pl.BlockSpec((1, D), lambda i: (0, 0))


def embed(h, tokens, patch_index, counts, table, gain_row, rows):
    steps = HALF // TILE
    grid_spec = pltpu.PrefetchScalarGridSpec(
        num_scalar_prefetch=3,
        grid=(steps,),
        in_specs=[
            pl.BlockSpec((TILE, D), lambda i, h, r, c: (h[0] * steps + i, 0)),
            pl.BlockSpec((TILE, 1), lambda i, h, r, c: (h[0] * steps + i, 0)),
            pl.BlockSpec((3 * GRID, 2048), lambda i, h, r, c: (0, 0)),
            pl.BlockSpec((1, D), lambda i, h, r, c: (0, 0)),
        ],
        out_specs=(VMEM, VMEM),
    )
    return pl.pallas_call(
        embed_body,
        grid_spec=grid_spec,
        out_shape=(pltpu.VMEM((HALF, D), jnp.float32), pltpu.VMEM((HALF, D), jnp.bfloat16)),
        compiler_params=pltpu.CompilerParams(vmem_limit_bytes=10 << 20),
        name="embed",
    )(jnp.full((1,), h, jnp.int32), rows, counts, hbm(tokens), patch_index, table, gain_row)


def norm(stream, branches, gain_row, rows, cols, last):
    out_specs = [VMEM, VMEM]
    out_shape = [pltpu.VMEM((HALF, D), jnp.float32), pltpu.VMEM((HALF, D), jnp.bfloat16)]
    tile = pl.BlockSpec((TILE, 1024), lambda i: (i, 0))
    if last:
        out_specs.append(tile)
        out_shape.append(jax.ShapeDtypeStruct((HALF, 1024), jnp.float32))
    return pl.pallas_call(
        norm_body,
        grid=(HALF // TILE,),
        in_specs=[SMEM, SMEM, VMEM, tile, tile, tile, tile, ROW],
        out_specs=out_specs,
        out_shape=out_shape,
        input_output_aliases={2: 0},
        compiler_params=pltpu.CompilerParams(vmem_limit_bytes=8 << 20),
        name="norm",
    )(rows, cols, stream, *branches, gain_row)


def matmul_body(spans, last, normed_ref, *refs):
    n = len(spans)
    weights, rest = refs[:n], refs[n:]
    out_ref, held = rest[-2:]
    at, pick = 0, []
    for w, (first, size) in zip(weights, spans):
        held[at : at + size, :] = w[...]
        pick.append(normed_ref[:, first : first + size])
        at += size
    left = pick[0] if at == size else jnp.concatenate(pick, axis=1)
    branch = jnp.dot(left, held[...], preferred_element_type=jnp.float32)
    if last == "part":
        out_ref[...] = branch
        return
    if last is None:
        out_ref[...] = branch.astype(jnp.bfloat16)
        return
    part_ref, stream_ref, counts_ref = rest[:3]
    slot = lax.broadcasted_iota(jnp.int32, (HALF, 1), 0) + last * HALF
    branch = (branch + part_ref[...]).astype(jnp.bfloat16)
    value = stream_ref[...] + branch.astype(jnp.float32)
    out_ref[...] = jnp.where(slot < counts_ref[0], value, 0.0).astype(jnp.bfloat16)


def matmul(normed, pieces, last=None, final=None):
    wide = 256
    spans = [(first, p.shape[0]) for p, first in pieces]
    depth = sum(size for _, size in spans)
    tile = pl.BlockSpec((HALF, wide), lambda i: (0, i))
    operands = [normed, *[p for p, _ in pieces]]
    in_specs = [VMEM] + [pl.BlockSpec((size, wide), lambda i: (0, i)) for _, size in spans]
    out_spec, aliases = tile, {}
    out_shape = jax.ShapeDtypeStruct((HALF, 1024), jnp.float32 if last == "part" else jnp.bfloat16)
    if final is not None:
        last, part, stream, counts, so_far = final
        h = last
        operands += [part, stream, counts]
        in_specs += [tile, tile, SMEM]
        out_spec = pl.BlockSpec((HALF, wide), lambda i: (h, i))
        out_shape = jax.ShapeDtypeStruct((2 * HALF, 1024), jnp.bfloat16)
        if so_far is not None:
            aliases = {len(operands): 0}
            operands.append(so_far)
            in_specs.append(pl.BlockSpec(memory_space=pl.ANY))
    return pl.pallas_call(
        functools.partial(matmul_body, spans, last),
        grid=(1024 // wide,),
        in_specs=in_specs,
        out_specs=out_spec,
        out_shape=out_shape,
        scratch_shapes=[pltpu.VMEM((depth, wide), jnp.bfloat16)],
        input_output_aliases=aliases,
        compiler_params=pltpu.CompilerParams(vmem_limit_bytes=12 << 20),
        name="project",
        cost_estimate=pl.CostEstimate(flops=2 * 256 * depth * 1024, transcendentals=0, bytes_accessed=depth << 11),
    )(*operands)


after = lambda x, *others: lax.optimization_barrier((x, *others))[0]


def per_device(
    tokens, counts, patch_index, clip_limit, norm_gain, params, moments, seconds, gradients
):
    squares = total(jnp.sum(gradients * gradients))
    places = [lax.axis_index(name).astype(jnp.int32) for name in EVERY]
    lanes = (jnp.arange(D // 4, dtype=jnp.int32), jnp.arange(GRID, dtype=jnp.int32))
    factor = jnp.minimum(1.0, clip_limit / (jnp.sqrt(squares) + 1e-06))
    head = adam_update(params[0], moments[0], seconds[0], gradients[0], factor)[0]
    head = head.astype(jnp.bfloat16)[None]
    params_new, moments_new, seconds_new, rest = adam(params, moments, seconds, gradients, factor)
    table = tables(lanes)
    rows, cols = row_blocks(*places[:3]), group_columns(*places[3:])

    partner = swap(head, "zh")
    lines = {}
    (line_a,) = first_phase(head, "x", 1)
    (line_b,) = first_phase(partner, "y", -1)
    lines[0] = (line_a, line_b)
    partner = swap(rest, "zh")

    near, far = {}, {}
    axis_of = ("y", "x")

    def open_layer(l, *waits):
        for color in (0, 1):
            x = after(lines[l][color], *waits) if waits else lines[l][color]
            for step in (1, -1):
                near[l, color, step] = shift(x, axis_of[color], step)

    def forward(l):
        step = 1 if l % 2 == 0 else -1
        for color in (0, 1):
            far[l, color] = [shift(near[l, color, step], axis_of[color], step)]

    def forward_both(l):
        for color in (0, 1):
            halves = []
            for step, part in ((1, slice(0, 256)), (-1, slice(256, 512))):
                halves.append(shift(near[l, color, step][part], axis_of[color], step))
            far[l, color] = halves

    open_layer(0)
    forward(0)
    line_a = first_phase(rest, "x", -1)
    line_b = first_phase(partner, "y", -1)
    for l in (1, 2, 3):
        lines[l] = (line_a[l - 1], line_b[l - 1])
    open_layer(1)
    forward(1)
    open_layer(2, near[1, 0, -1], near[1, 1, -1])
    forward(2)
    open_layer(3, near[2, 0, 1], near[2, 1, 1])
    forward_both(3)

    streams, branches = [None, None], [None, None]
    mixed = None
    patch_index = patch_index[:, None]
    for l in range(LAYERS):
        pieces, late, at = [], [], 0
        for color in (0, 1):
            for p in (lines[l][color], near[l, color, 1], near[l, color, -1], *far[l, color]):
                (late if p.shape[0] < 512 else pieces).append((p, at))
                at += p.shape[0]
        gain_row = norm_gain[l][None, :]
        last = l + 1 == LAYERS
        for h in (0, 1):
            if l == 0:
                streams[h], normed = embed(h, tokens, patch_index, counts, table, gain_row, rows)
            else:
                streams[h], normed, *mine = norm(
                    streams[h], branches[h], gain_row, rows, cols, last
                )
            if last:
                part = matmul(normed, pieces, "part")
                mixed = matmul(normed, late, None, (h, part, mine[0], counts, mixed))
                continue
            branch = matmul(normed, pieces)
            across = swap(branch, "zl")
            beside = swap(branch, "core")
            both = swap(across, "core")
            branches[h] = (branch, beside, across, both)
    return (params_new, moments_new, seconds_new, mixed)


def solution(mesh):
    split = Mesh(mesh.devices.reshape(2, 4, 4, 2, 2), EVERY)
    return jax.shard_map(
        per_device,
        mesh=split,
        in_specs=(
            P(DP, None),
            P(DP),
            P(DP),
            P(),
            P(),
            P(None, DP, FSDP),
            P(None, DP, FSDP),
            P(None, DP, FSDP),
            P(None, DP, FSDP),
        ),
        out_specs=(P(None, DP, FSDP), P(None, DP, FSDP), P(None, DP, FSDP), P(DP, FSDP)),
        check_vma=False,
    )
```

```python
import functools

import jax
import jax.numpy as jnp
from jax import lax
from jax.experimental import pallas as pl
from jax.experimental.pallas import tpu as pltpu
from jax.sharding import Mesh
from jax.sharding import PartitionSpec as P

D = 4096
LAYERS = 4
GRID = 16
STEP = 40
BLK = 128
FSDP = ("zl", "core")
DP = ("zh", "y", "x")
EVERY = ("zh", "y", "x", "zl", "core")

beta_one = 0.9
beta_two = 0.95
adam_eps = 1e-08
learning_rate = 0.0024
weight_decay = 0.05
norm_eps = 1e-06


def shift(x, axis, step, size=4):
    return lax.ppermute(x, axis, [(i, (i + step) % size) for i in range(size)])


def swap(x, axis):
    return lax.ppermute(x, axis, [(0, 1), (1, 0)])


def spread_all(x):
    spread = jnp.broadcast_to(x.reshape(1, 1), (128, 128))
    return lax.all_to_all(spread, EVERY, 0, 0, tiled=True)


def adam_update(params, moments, seconds, gradients, factor):
    clipped = gradients * factor
    moments_new = beta_one * moments + (1.0 - beta_one) * clipped
    seconds_new = beta_two * seconds + (1.0 - beta_two) * clipped * clipped
    direction = (
        moments_new
        / (1.0 - beta_one**STEP)
        / (jnp.sqrt(seconds_new / (1.0 - beta_two**STEP)) + adam_eps)
    )
    params_new = params - learning_rate * (direction + weight_decay * params)
    return (params_new, moments_new, seconds_new)


STRIP = 16


def hbm(x):
    return pltpu.with_memory_space_constraint(x, pltpu.MemorySpace.HBM)


def head_body(clip_ref, squares_ref, *refs):
    factor_ref, weights_ref = refs[4:]
    squares = jnp.sum(squares_ref[:, 0:1], axis=0, keepdims=True)
    factor = jnp.minimum(1.0, clip_ref[0] / (jnp.sqrt(squares) + 1e-06))
    factor_ref[0] = factor[0, 0]

    def strip(j, carry):
        at = pl.ds(pl.multiple_of(j * STRIP, STRIP), STRIP)
        new = adam_update(*[r[0, at, :] for r in refs[:4]], factor)[0]
        weights_ref[0, at, :] = new.astype(jnp.bfloat16)
        return carry

    lax.fori_loop(0, BLK // STRIP, strip, 0)


def first_weights(squares, clip_limit, *state):
    first = pl.BlockSpec((1, BLK, 1024), lambda i: (0, 0, 0))
    smem = pl.BlockSpec(memory_space=pltpu.SMEM)
    return pl.pallas_call(
        head_body,
        grid=(1,),
        in_specs=[smem, pl.BlockSpec((128, 128), lambda i: (0, 0))] + [first] * 4,
        out_specs=[smem, first],
        out_shape=[
            jax.ShapeDtypeStruct((1,), jnp.float32),
            jax.ShapeDtypeStruct((1, BLK, 1024), jnp.bfloat16),
        ],
        compiler_params=pltpu.CompilerParams(vmem_limit_bytes=8 << 20),
        name="head",
    )(clip_limit.reshape(1), squares, *[hbm(x) for x in state])


def adam_body(factor_ref, *refs):
    ins, outs, weights_ref = refs[:4], refs[4:7], refs[7]
    held, rounded, taken, given = refs[8:12], refs[12], refs[13], refs[14]
    fetch = lambda a, l: pltpu.make_async_copy(ins[a].at[l], held[a].at[l], taken.at[a, l])
    store = lambda a, l: pltpu.make_async_copy(held[a].at[l], outs[a].at[l], given.at[a, l])

    def begin(l, carry):
        for a in range(4):
            fetch(a, l).start()
        return carry

    lax.fori_loop(0, LAYERS, begin, 0)

    def layer(l, carry):
        for a in range(4):
            fetch(a, l).wait()

        def strip(j, carry):
            at = pl.ds(pl.multiple_of(j * STRIP, STRIP), STRIP)
            new = adam_update(*[h[l, at, :] for h in held], factor_ref[0])
            for a in range(3):
                held[a][l, at, :] = new[a]
            rounded[jnp.maximum(l - 1, 0), at, :] = new[0].astype(jnp.bfloat16)
            return carry

        lax.fori_loop(0, BLK // STRIP, strip, 0)
        for a in range(3):
            store(a, l).start()
        return carry

    def finish(l, carry):
        for a in range(3):
            store(a, l).wait()
        return carry

    lax.fori_loop(0, LAYERS, layer, 0)
    every = pltpu.make_async_copy(rounded, weights_ref, given.at[3, 0])
    every.start()
    lax.fori_loop(0, LAYERS, finish, 0)
    every.wait()


def adam(params, moments, seconds, gradients, factor):
    any_space = pl.BlockSpec(memory_space=pltpu.MemorySpace.HBM)
    whole = jax.ShapeDtypeStruct(params.shape, jnp.float32)
    rest = jax.ShapeDtypeStruct((LAYERS - 1, BLK, 1024), jnp.bfloat16)
    return pl.pallas_call(
        adam_body,
        in_specs=[pl.BlockSpec(memory_space=pltpu.SMEM)] + [any_space] * 4,
        out_specs=[any_space] * 4,
        out_shape=[whole] * 3 + [rest],
        scratch_shapes=[pltpu.VMEM(params.shape, jnp.float32)] * 4
        + [
            pltpu.VMEM(rest.shape, jnp.bfloat16),
            pltpu.SemaphoreType.DMA((4, LAYERS)),
            pltpu.SemaphoreType.DMA((4, LAYERS)),
        ],
        compiler_params=pltpu.CompilerParams(vmem_limit_bytes=12 << 20),
        name="adam",
    )(factor, *[hbm(x) for x in (params, moments, seconds, gradients)])


def tables(lanes):
    quarter = D // 4
    freqs = 1.0 / 10000.0 ** (lanes[0].astype(jnp.float32) / quarter)
    angle = lanes[1].astype(jnp.float32)[:, None] * freqs[None, :]
    table = jnp.concatenate([jnp.sin(angle), jnp.cos(angle)], axis=1)
    high = lax.reduce_precision(table, 8, 7)
    middle = lax.reduce_precision(table - high, 8, 7)
    low = table - high - middle
    return jnp.concatenate([high, middle, low], axis=0).astype(jnp.bfloat16)


def join_body(n, *refs):
    for j, out in enumerate(refs[-n:]):
        for k, part in enumerate(refs[:-n]):
            out[k * BLK : (k + 1) * BLK, :] = part[j]


def join(parts):
    n, tall = parts[0].shape[0], len(parts) * BLK
    wide = 512
    return pl.pallas_call(
        functools.partial(join_body, n),
        grid=(1024 // wide,),
        in_specs=[pl.BlockSpec((n, BLK, wide), lambda i: (0, 0, i))] * len(parts),
        out_specs=[pl.BlockSpec((tall, wide), lambda i: (0, i))] * n,
        out_shape=[jax.ShapeDtypeStruct((tall, 1024), jnp.bfloat16)] * n,
        compiler_params=pltpu.CompilerParams(vmem_limit_bytes=12 << 20),
        name="join",
    )(*parts)


def first_phase(x, axis, step, split=False):
    ahead = shift(x, axis, step)
    behind = shift(x, axis, -step)
    far = shift(ahead, axis, step)
    prev, next_ = (ahead, behind) if step == 1 else (behind, ahead)
    if split:
        return join((x, prev))[0], join((next_, far))[0]
    return join((x, prev, next_, far))


def row_blocks(zh, y, x):
    order = jnp.array([0, 3, 1, 2], jnp.int32)
    ys, xs = (y + order) % 4, (x + order) % 4
    first = zh * 16 + ys[:, None] * 4 + xs[None, :]
    second = (1 - zh) * 16 + ys[None, :] * 4 + xs[:, None]
    return jnp.concatenate([first.reshape(-1), second.reshape(-1)])


def group_columns(zl, core):
    flips = jnp.arange(4, dtype=jnp.int32)
    return (zl * 2 + core) ^ flips


def normalize(at, rows_ref, stream_ref, gain_ref, normed_ref):
    stream = stream_ref[at, :]
    centre = jnp.sum(stream, axis=1, keepdims=True) * (1.0 / D)
    shifted = stream - centre
    spread = jnp.sum(shifted * shifted, axis=1, keepdims=True) * (1.0 / D)
    scale = lax.rsqrt(spread + norm_eps)
    for j in range(D // BLK):
        col = pl.ds(pl.multiple_of(rows_ref[j] * BLK, BLK), BLK)
        piece = (stream_ref[at, col] - centre) * scale * gain_ref[:, col]
        normed_ref[at, j * BLK : (j + 1) * BLK] = piece.astype(jnp.bfloat16)


TILE = 64
EMBED_TILE = 32
HALF = 256


def tile_rows(tile):
    return pl.ds(pl.multiple_of(pl.program_id(0) * tile, tile), tile)


def embed_body(half_ref, rows_ref, counts_ref, tokens_ref, patch_ref, table_ref, gain_ref, stream_ref, normed_ref):
    at = tile_rows(EMBED_TILE)
    patch = patch_ref[...]
    lanes = lax.broadcasted_iota(jnp.int32, (EMBED_TILE, 3 * GRID), 1) & (GRID - 1)
    first = half_ref[0] * HALF + pl.program_id(0) * EMBED_TILE
    valid = lax.broadcasted_iota(jnp.int32, (EMBED_TILE, 1), 0) + first < counts_ref[0]
    for side, where in enumerate((patch >> 4, patch & (GRID - 1))):
        pick = jnp.where(where == lanes, 1.0, 0.0).astype(jnp.bfloat16)
        code = jnp.dot(pick, table_ref[...], preferred_element_type=jnp.float32)
        cols = slice(side * 2048, side * 2048 + 2048)
        value = tokens_ref[:, cols].astype(jnp.float32) + code
        stream_ref[at, cols] = jnp.where(valid, value, 0.0)
    normalize(at, rows_ref, stream_ref, gain_ref, normed_ref)


def norm_body(rows_ref, cols_ref, stream_in, b0, b1, b2, b3, gain_ref, stream_ref, normed_ref):
    at = tile_rows(TILE)
    for j, branch in enumerate((b0, b1, b2, b3)):
        col = pl.ds(pl.multiple_of(cols_ref[j] * 1024, 1024), 1024)
        stream_ref[at, col] = stream_in[at, col] + branch[...].astype(jnp.float32)
    normalize(at, rows_ref, stream_ref, gain_ref, normed_ref)


SMEM = pl.BlockSpec(memory_space=pltpu.SMEM)
VMEM = pl.BlockSpec(memory_space=pltpu.VMEM)
ROW = pl.BlockSpec((1, D), lambda i: (0, 0))


def embed(h, tokens, patch_index, counts, table, gain_row, rows):
    steps = HALF // EMBED_TILE
    grid_spec = pltpu.PrefetchScalarGridSpec(
        num_scalar_prefetch=3,
        grid=(steps,),
        in_specs=[
            pl.BlockSpec((EMBED_TILE, D), lambda i, h, r, c: (h[0] * steps + i, 0)),
            pl.BlockSpec((EMBED_TILE, 1), lambda i, h, r, c: (h[0] * steps + i, 0)),
            pl.BlockSpec((3 * GRID, 2048), lambda i, h, r, c: (0, 0)),
            pl.BlockSpec((1, D), lambda i, h, r, c: (0, 0)),
        ],
        out_specs=(VMEM, VMEM),
    )
    return pl.pallas_call(
        embed_body,
        grid_spec=grid_spec,
        out_shape=(pltpu.VMEM((HALF, D), jnp.float32), pltpu.VMEM((HALF, D), jnp.bfloat16)),
        compiler_params=pltpu.CompilerParams(vmem_limit_bytes=10 << 20),
        name="embed",
    )(jnp.full((1,), h, jnp.int32), rows, counts, hbm(tokens), patch_index, table, gain_row)


def norm(stream, branches, gain_row, rows, cols):
    out_specs = [VMEM, VMEM]
    out_shape = [pltpu.VMEM((HALF, D), jnp.float32), pltpu.VMEM((HALF, D), jnp.bfloat16)]
    tile = pl.BlockSpec((TILE, 1024), lambda i: (i, 0))
    return pl.pallas_call(
        norm_body,
        grid=(HALF // TILE,),
        in_specs=[SMEM, SMEM, VMEM, tile, tile, tile, tile, ROW],
        out_specs=out_specs,
        out_shape=out_shape,
        input_output_aliases={2: 0},
        compiler_params=pltpu.CompilerParams(vmem_limit_bytes=8 << 20),
        name="norm",
    )(rows, cols, stream, *branches, gain_row)


def matmul_body(spans, kind, *refs):
    n = len(spans)
    lefts = 2 if kind == "final" else 1
    normed, weights, rest = refs[:lefts], refs[lefts : lefts + n], refs[lefts + n :]
    out_ref, held = rest[-2:]
    at = 0
    for w, (_, size) in zip(weights, spans):
        held[at : at + size, :] = w[...]
        at += size
    cols = pl.ds(pl.multiple_of(pl.program_id(0) * 256, 256), 256)
    for h, normed_ref in enumerate(normed):
        if at == D:
            left = normed_ref[...]
        else:
            left = jnp.concatenate([normed_ref[:, p : p + size] for p, size in spans], axis=1)
        branch = jnp.dot(left, held[...], preferred_element_type=jnp.float32)
        if kind == "part":
            out_ref[:, cols] = branch
        elif kind == "whole":
            out_ref[...] = branch.astype(jnp.bfloat16)
        else:
            parts, streams, (cols_ref, counts_ref) = rest[:2], rest[2:4], rest[4:6]
            mine = pl.ds(pl.multiple_of(cols_ref[0] * 1024 + pl.program_id(0) * 256, 256), 256)
            slot = lax.broadcasted_iota(jnp.int32, (HALF, 1), 0) + h * HALF
            branch = (branch + parts[h][:, cols]).astype(jnp.bfloat16)
            value = streams[h][:, mine] + branch.astype(jnp.float32)
            value = jnp.where(slot < counts_ref[0], value, 0.0)
            out_ref[h * HALF : (h + 1) * HALF, :] = value.astype(jnp.bfloat16)


def matmul(normed, pieces, kind="whole", extra=()):
    wide = 256
    spans = [(first, p.shape[0]) for p, first in pieces]
    depth = sum(size for _, size in spans)
    rows = HALF * len(normed)
    in_specs = [VMEM] * len(normed)
    in_specs += [pl.BlockSpec((size, wide), lambda i: (0, i)) for _, size in spans]
    in_specs += [VMEM] * 4 + [SMEM] * 2 if extra else []
    out_spec = pl.BlockSpec((rows, wide), lambda i: (0, i))
    out_shape = jax.ShapeDtypeStruct((rows, 1024), jnp.bfloat16)
    if kind == "part":
        out_spec, out_shape = VMEM, pltpu.VMEM((rows, 1024), jnp.float32)
    return pl.pallas_call(
        functools.partial(matmul_body, spans, kind),
        grid=(1024 // wide,),
        in_specs=in_specs,
        out_specs=out_spec,
        out_shape=out_shape,
        scratch_shapes=[pltpu.VMEM((depth, wide), jnp.bfloat16)],
        compiler_params=pltpu.CompilerParams(vmem_limit_bytes=12 << 20),
        name="project",
        cost_estimate=pl.CostEstimate(
            flops=2 * rows * depth * 1024, transcendentals=0, bytes_accessed=depth << 11
        ),
    )(*normed, *[p for p, _ in pieces], *extra)


after = lambda x, *others: lax.optimization_barrier((x, *others))[0]


def per_device(
    tokens, counts, patch_index, clip_limit, norm_gain, params, moments, seconds, gradients
):
    squares = spread_all(jnp.sum(gradients * gradients))
    places = [lax.axis_index(name).astype(jnp.int32) for name in EVERY]
    lanes = (jnp.arange(D // 4, dtype=jnp.int32), jnp.arange(GRID, dtype=jnp.int32))
    table = tables(lanes)
    rows, cols = row_blocks(*places[:3]), group_columns(*places[3:])
    factor, head = first_weights(squares, clip_limit, params, moments, seconds, gradients)
    params_new, moments_new, seconds_new, rest = adam(params, moments, seconds, gradients, factor)
    partner = swap(head, "zh")
    lines = {}
    line_a = first_phase(head, "x", 1, split=True)
    line_b = first_phase(partner, "y", 1)
    lines[0] = (line_a, line_b)
    partner = swap(rest, "zh")

    near, far = {}, {}
    axis_of = ("y", "x")

    def open_layer(l, *waits):
        for color in (0, 1):
            for step in (1, -1):
                near[l, color, step] = []
            for x in lines[l][color]:
                x = after(x, *waits) if waits else x
                for step in (1, -1):
                    near[l, color, step].append(shift(x, axis_of[color], step))

    def forward(l):
        step = 1 if l % 2 == 0 else -1
        for color in (0, 1):
            far[l, color] = [shift(x, axis_of[color], step) for x in near[l, color, step]]

    def forward_both(l):
        for color in (0, 1):
            halves = []
            for step, part in ((1, slice(0, 256)), (-1, slice(256, 512))):
                halves.append(shift(near[l, color, step][0][part], axis_of[color], step))
            far[l, color] = halves

    open_layer(0)
    forward(0)
    line_a = first_phase(rest, "x", -1)
    line_b = first_phase(partner, "y", -1)
    for l in (1, 2, 3):
        lines[l] = ((line_a[l - 1],), (line_b[l - 1],))
    open_layer(1)
    forward(1)
    open_layer(2, near[1, 0, -1][0], near[1, 1, -1][0])
    forward(2)
    open_layer(3, near[2, 0, 1][0], near[2, 1, 1][0])
    forward_both(3)

    streams, branches = [None, None], [None, None]
    parts, lefts = [], []
    patch_index = patch_index[:, None]
    for l in range(LAYERS):
        last = l + 1 == LAYERS
        pieces, late, at = [], [], 0
        for color in (0, 1):
            for p in (*lines[l][color], *near[l, color, 1], *near[l, color, -1], *far[l, color]):
                (late if last and p.shape[0] < 512 else pieces).append((p, at))
                at += p.shape[0]
        gain_row = norm_gain[l][None, :]
        for h in (0, 1):
            if l == 0:
                streams[h], normed = embed(h, tokens, patch_index, counts, table, gain_row, rows)
            else:
                streams[h], normed = norm(
                    streams[h], branches[h], gain_row, rows, cols
                )
            if last:
                parts.append(matmul((normed,), pieces, "part"))
                lefts.append(normed)
                continue
            branch = matmul((normed,), pieces)
            across = swap(branch, "zl")
            beside = swap(branch, "core")
            both = swap(across, "core")
            branches[h] = (branch, beside, across, both)
    mixed = matmul(lefts, late, "final", (*parts, *streams, cols, counts))
    return (params_new, moments_new, seconds_new, mixed)


def solution(mesh):
    split = Mesh(mesh.devices.reshape(2, 4, 4, 2, 2), EVERY)
    return jax.shard_map(
        per_device,
        mesh=split,
        in_specs=(
            P(DP, None),
            P(DP),
            P(DP),
            P(),
            P(),
            P(None, DP, FSDP),
            P(None, DP, FSDP),
            P(None, DP, FSDP),
            P(None, DP, FSDP),
        ),
        out_specs=(P(None, DP, FSDP), P(None, DP, FSDP), P(None, DP, FSDP), P(DP, FSDP)),
        check_vma=False,
    )
```
